16 devices in a mesh: dp: 2 (over y, z), tp: 8 (over x, core).
Axes of the slice: x: 4, y: 2, z: 1, core: 2. Of those that a mesh axis runs over, the one named last changes fastest.
The devices are a block of a 4x4x8 slice.
Arguments:
- x_in: bfloat16 [2, 4096, 2048], P('dp', 'tp'), parts along dimension 0
- cond_vec: bfloat16 [2, 2048], P('dp'), parts along dimension 0
- rope_cos: float32 [4096, 128], P('tp')
- rope_sin: float32 [4096, 128], P('tp')
- w_mod: bfloat16 [2, 2048, 6144], replicated
- b_mod: bfloat16 [2, 6144], replicated
- w_in: bfloat16 [2, 2048, 8, 1792], P(None, None, 'tp')
- b_in: bfloat16 [2, 8, 1792], P(None, 'tp')
- q_scale: bfloat16 [2, 256], replicated
- k_scale: bfloat16 [2, 256], replicated
- w_out: bfloat16 [2, 8, 1280, 2048], P(None, 'tp')
- b_out: bfloat16 [2, 2048], replicated
- d_out: bfloat16 [2, 4096, 2048], P('dp', 'tp'), parts along dimension 0
Outputs:
- output 1: bfloat16 [2, 4096, 2048], P('dp', 'tp'), parts along dimension 0
- output 2: bfloat16 [2, 4096, 2048], P('dp', 'tp'), parts along dimension 0
- output 3: float32 [4, 2048, 6144], P('dp'), parts along dimension 0
- output 4: float32 [4, 6144], P('dp'), parts along dimension 0
- output 5: bfloat16 [4, 2048, 8, 1792], P('dp', None, 'tp'), parts along dimension 0
- output 6: float32 [4, 8, 1792], P('dp', 'tp'), parts along dimension 0
- output 7: float32 [4, 256], P('dp'), parts along dimension 0
- output 8: float32 [4, 256], P('dp'), parts along dimension 0
- output 9: bfloat16 [4, 8, 1280, 2048], P('dp', 'tp'), parts along dimension 0
- output 10: float32 [4, 2048], P('dp'), parts along dimension 0
There are 2 independent parts. The reference program is written for one: setup_inputs(seed, part) draws one part's arguments, and reference() takes and returns one part's arrays. A program takes and returns all parts, laid end to end along the dimension named above; an argument that names none is the same for every part.
All inputs are finite; a program needn't handle non-finite values.
Results may differ from the reference program's by a relative error of at most 0.02.
Values are sent between devices in bfloat16 or wider.
A program may use at most 768 MiB of HBM per device.

```python
import jax
import jax.numpy as jnp
from jax import lax

MODEL_DIM = 2048
NUM_HEADS = 8
HEAD_DIM = 256
MLP_DIM = 8192
SEQ_LEN = 4096
BATCH_SIZE = 1
NUM_BLOCKS = 2

GROUP_MLP = MLP_DIM // NUM_HEADS
GROUP_COLS = 3 * HEAD_DIM + GROUP_MLP
GROUP_ROWS = HEAD_DIM + GROUP_MLP
TEXT_LEN = SEQ_LEN // 4
HALF_DIM = HEAD_DIM // 2
NORM_EPS = 1e-6


def rope_tables(table_key):
    key_w, key_r, key_c = jax.random.split(table_key, 3)
    grid_width = jax.random.randint(key_w, (), 8, 65)
    row_off = jax.random.randint(key_r, (), 0, 32)
    col_off = jax.random.randint(key_c, (), 0, 32)
    token_idx = jnp.arange(SEQ_LEN) - TEXT_LEN
    is_image = token_idx >= 0
    safe_idx = jnp.maximum(token_idx, 0)
    row_pos = jnp.where(is_image, safe_idx // grid_width + row_off, 0).astype(jnp.float32)
    col_pos = jnp.where(is_image, safe_idx % grid_width + col_off, 0).astype(jnp.float32)
    n_zero = HALF_DIM // 8
    n_row = (HALF_DIM - n_zero) // 2
    n_col = HALF_DIM - n_zero - n_row
    freq_row = 10000.0 ** (-jnp.arange(n_row, dtype=jnp.float32) / n_row)
    freq_col = 10000.0 ** (-jnp.arange(n_col, dtype=jnp.float32) / n_col)
    angles = jnp.concatenate([jnp.zeros((SEQ_LEN, n_zero), jnp.float32), row_pos[:, None] * freq_row[None, :], col_pos[:, None] * freq_col[None, :]], axis=1)
    return jnp.cos(angles), jnp.sin(angles)


def setup_inputs(seed: int = 0, part: int = 0) -> dict:
    base_key = jax.random.key(seed)
    shared_keys = jax.random.split(base_key, 12)
    own_keys = jax.random.split(jax.random.fold_in(base_key, part), 4)
    is_text = (jnp.arange(SEQ_LEN) < TEXT_LEN)[None, :, None]
    x_raw = jax.random.normal(own_keys[0], (BATCH_SIZE, SEQ_LEN, MODEL_DIM), jnp.float32)
    text_shift = 0.8 * jax.random.normal(own_keys[1], (MODEL_DIM,), jnp.float32)
    x_in = jnp.where(is_text, 0.6 * x_raw + text_shift, x_raw)
    cond_vec = jax.random.normal(own_keys[2], (BATCH_SIZE, MODEL_DIM), jnp.float32)
    d_out = jax.random.normal(own_keys[3], (BATCH_SIZE, SEQ_LEN, MODEL_DIM), jnp.float32)
    rope_cos, rope_sin = rope_tables(shared_keys[0])
    w_mod = jax.random.normal(shared_keys[1], (NUM_BLOCKS, MODEL_DIM, 3 * MODEL_DIM), jnp.float32) * MODEL_DIM ** -0.5
    b_mod = 0.5 * jax.random.normal(shared_keys[2], (NUM_BLOCKS, 3 * MODEL_DIM), jnp.float32)
    w_in = jax.random.normal(shared_keys[3], (NUM_BLOCKS, MODEL_DIM, NUM_HEADS, GROUP_COLS), jnp.float32) * MODEL_DIM ** -0.5
    b_in = 0.3 * jax.random.normal(shared_keys[4], (NUM_BLOCKS, NUM_HEADS, GROUP_COLS), jnp.float32)
    q_scale = 1.5 + 0.4 * jax.random.normal(shared_keys[5], (NUM_BLOCKS, HEAD_DIM), jnp.float32)
    k_scale = 1.5 + 0.4 * jax.random.normal(shared_keys[6], (NUM_BLOCKS, HEAD_DIM), jnp.float32)
    w_out = jax.random.normal(shared_keys[7], (NUM_BLOCKS, NUM_HEADS, GROUP_ROWS, MODEL_DIM), jnp.float32) * (MODEL_DIM + MLP_DIM) ** -0.5
    b_out = 0.3 * jax.random.normal(shared_keys[8], (NUM_BLOCKS, MODEL_DIM), jnp.float32)
    return {"x_in": x_in.astype(jnp.bfloat16), "cond_vec": cond_vec.astype(jnp.bfloat16), "rope_cos": rope_cos, "rope_sin": rope_sin, "w_mod": w_mod.astype(jnp.bfloat16), "b_mod": b_mod.astype(jnp.bfloat16), "w_in": w_in.astype(jnp.bfloat16), "b_in": b_in.astype(jnp.bfloat16), "q_scale": q_scale.astype(jnp.bfloat16), "k_scale": k_scale.astype(jnp.bfloat16), "w_out": w_out.astype(jnp.bfloat16), "b_out": b_out.astype(jnp.bfloat16), "d_out": d_out.astype(jnp.bfloat16)}


def to_bf16(tensor):
    return tensor.astype(jnp.bfloat16).astype(jnp.float32)


def rms_norm(tensor):
    return tensor * lax.rsqrt(jnp.mean(tensor * tensor, axis=-1, keepdims=True) + NORM_EPS)


def layer_norm(tensor):
    row_mean = jnp.mean(tensor, axis=-1, keepdims=True)
    centered = tensor - row_mean
    row_var = jnp.mean(centered * centered, axis=-1, keepdims=True)
    return centered * lax.rsqrt(row_var + NORM_EPS)


def apply_rope(tensor, rope_cos, rope_sin):
    pair_view = tensor.reshape(tensor.shape[:-1] + (tensor.shape[-1] // 2, 2))
    even_part = pair_view[..., 0]
    odd_part = pair_view[..., 1]
    cos_wide = rope_cos[None, :, None, :]
    sin_wide = rope_sin[None, :, None, :]
    rotated = jnp.stack([even_part * cos_wide - odd_part * sin_wide, even_part * sin_wide + odd_part * cos_wide], axis=-1)
    return rotated.reshape(tensor.shape)


def head_attention(operands):
    q_head, k_head, v_head = operands
    scores = jnp.einsum("bqe,bke->bqk", q_head, k_head) * (HEAD_DIM ** -0.5)
    attn_probs = jax.nn.softmax(scores, axis=-1)
    return to_bf16(jnp.einsum("bqk,bke->bqe", to_bf16(attn_probs), v_head))


def block_forward(x_f32, silu_vec, rope_cos, rope_sin, layer_params):
    w_mod, b_mod, w_in, b_in, q_scale, k_scale, w_out, b_out = layer_params
    mod_vec = jnp.dot(silu_vec, w_mod, preferred_element_type=jnp.float32) + b_mod
    mod_shift, mod_scale, mod_gate = jnp.split(mod_vec, 3, axis=-1)
    normed = to_bf16(layer_norm(x_f32) * (1.0 + mod_scale[:, None, :]) + mod_shift[:, None, :])
    projected = jnp.einsum("bsd,dhc->bshc", normed, w_in) + b_in
    q_rot = to_bf16(apply_rope(rms_norm(projected[..., :HEAD_DIM]) * q_scale, rope_cos, rope_sin))
    k_rot = to_bf16(apply_rope(rms_norm(projected[..., HEAD_DIM:2 * HEAD_DIM]) * k_scale, rope_cos, rope_sin))
    v_part = to_bf16(projected[..., 2 * HEAD_DIM:3 * HEAD_DIM])
    mlp_act = to_bf16(jax.nn.gelu(projected[..., 3 * HEAD_DIM:], approximate=True))
    per_head = lax.map(jax.checkpoint(head_attention), (jnp.moveaxis(q_rot, 2, 0), jnp.moveaxis(k_rot, 2, 0), jnp.moveaxis(v_part, 2, 0)))
    attn_out = jnp.moveaxis(per_head, 0, 2)
    joined = jnp.concatenate([attn_out, mlp_act], axis=-1)
    mixed_out = jnp.einsum("bshc,hcd->bsd", joined, w_out)
    return to_bf16(x_f32 + mod_gate[:, None, :] * (mixed_out + b_out))


def reference(x_in, cond_vec, rope_cos, rope_sin, w_mod, b_mod, w_in, b_in, q_scale, k_scale, w_out, b_out, d_out):
    silu_vec = to_bf16(jax.nn.silu(cond_vec.astype(jnp.float32)))
    weights = tuple(weight.astype(jnp.float32) for weight in (w_mod, b_mod, w_in, b_in, q_scale, k_scale, w_out, b_out))

    def stack_forward(x_f32, all_params):
        def layer_step(state_in, layer_params):
            return block_forward(state_in, silu_vec, rope_cos, rope_sin, layer_params), None
        final_state, unused = lax.scan(layer_step, x_f32, all_params)
        return final_state

    out_f32, pullback = jax.vjp(stack_forward, x_in.astype(jnp.float32), weights)
    grad_x, grad_w = pullback(d_out.astype(jnp.float32))
    return (out_f32.astype(jnp.bfloat16), grad_x.astype(jnp.bfloat16), grad_w[0], grad_w[1], grad_w[2].astype(jnp.bfloat16), grad_w[3], grad_w[4], grad_w[5], grad_w[6].astype(jnp.bfloat16), grad_w[7])
```

```python
import functools
import jax
import jax.numpy as jnp
from jax import lax
from jax.sharding import PartitionSpec as P
from jax.experimental import pallas as pl
from jax.experimental.pallas import tpu as pltpu

NORM_EPS = 1e-6
NUM_CHUNKS = 2
TILE = 512
F32 = jnp.float32
BF16 = jnp.bfloat16
LANES = 128
GELU_A = 0.7978845608028654
GELU_B = 0.044715


def call(body, **kw):
    flops = kw.pop("flops")
    nbytes = kw.pop("nbytes")
    kw["cost_estimate"] = pl.CostEstimate(flops=int(flops), bytes_accessed=int(nbytes), transcendentals=0)
    kw["compiler_params"] = pltpu.CompilerParams(dimension_semantics=("arbitrary",), vmem_limit_bytes=60 * 1024 * 1024)
    return pl.pallas_call(body, **kw)


def full(shape):
    return pl.BlockSpec(shape, lambda i: (0,) * len(shape))


def rows(tile, cols):
    return pl.BlockSpec((tile, cols), lambda i: (i, 0))


def dot(a, b, dims=((1,), (0,))):
    return lax.dot_general(a, b, (dims, ((), ())), preferred_element_type=F32)


def as_row(col):
    return jnp.broadcast_to(col, (col.shape[0], LANES)).T[:8]


def inproj_body(h_ref, w_ref, b_ref, qs_ref, ks_ref, cs_ref, q_ref, k_ref, v_ref, j_ref, yqk_ref, u_ref):
    hd = q_ref.shape[1]
    half = hd // 2
    h = h_ref[...]
    cos = cs_ref[:, :half]
    sin = cs_ref[:, half:]
    for part, (s_ref, o_ref, post) in enumerate(((qs_ref, q_ref, hd ** -0.5), (ks_ref, k_ref, None))):
        lo = part * hd
        y = dot(h, w_ref[:, lo:lo + hd]) + b_ref[:, lo:lo + hd]
        yqk_ref[:, lo:lo + hd] = y
        inv = lax.rsqrt(jnp.mean(y * y, axis=-1, keepdims=True) + NORM_EPS)
        t = y * inv * s_ref[...]
        ta, tb = t[:, :half], t[:, half:]
        ra = ta * cos - tb * sin
        rb = ta * sin + tb * cos
        ra = ra.astype(BF16)
        rb = rb.astype(BF16)
        if post is not None:
            ra = ra * BF16(post)
            rb = rb * BF16(post)
        o_ref[:, :half] = ra
        o_ref[:, half:] = rb
    v_ref[...] = (dot(h, w_ref[:, 2 * hd:3 * hd]) + b_ref[:, 2 * hd:3 * hd]).astype(BF16)
    j_ref[:, :hd] = jnp.zeros((h.shape[0], hd), BF16)
    mlp = u_ref.shape[1]
    for lo in range(0, mlp, 256):
        c0 = 3 * hd + lo
        u = dot(h, w_ref[:, c0:c0 + 256]) + b_ref[:, c0:c0 + 256]
        u_ref[:, lo:lo + 256] = u
        g = 0.5 * u * (1.0 + jnp.tanh(GELU_A * (u + GELU_B * (u * u * u))))
        j_ref[:, hd + lo:hd + lo + 256] = g.astype(BF16)


def inproj(h, w, b, qs, ks, cs):
    s, d = h.shape
    n = w.shape[1]
    hd = qs.shape[1]
    mlp = n - 3 * hd
    tile = min(TILE, s)
    return call(
        inproj_body,
        grid=(s // tile,),
        in_specs=[rows(tile, d), full((d, n)), full((1, n)), full((1, hd)), full((1, hd)), rows(tile, hd)],
        out_specs=[rows(tile, hd)] * 3 + [rows(tile, hd + mlp), rows(tile, 2 * hd), rows(tile, mlp)],
        out_shape=[jax.ShapeDtypeStruct((s, hd), BF16)] * 3
        + [jax.ShapeDtypeStruct((s, hd + mlp), BF16), jax.ShapeDtypeStruct((s, 2 * hd), F32), jax.ShapeDtypeStruct((s, mlp), F32)],
        flops=2 * s * d * n,
        nbytes=s * d * 2 + d * n * 2 + s * n * 6,
        name="inproj",
    )(h, w, b, qs, ks, cs)


def attn_body(nc, bk, q_ref, *refs):
    k_refs, v_refs, _, o_ref, lse_ref = refs[:nc], refs[nc:2 * nc], refs[2 * nc], refs[2 * nc + 1], refs[2 * nc + 2]
    q = q_ref[...]
    pieces = [(c, lo) for c in range(nc) for lo in range(0, k_refs[0].shape[0], bk)]

    def score(idx):
        c, lo = pieces[idx]
        return dot(q, k_refs[c][lo:lo + bk, :], ((1,), (1,)))

    m = l = acc = None
    s_next = score(0)
    for idx, (c, lo) in enumerate(pieces):
        s = s_next
        if idx + 1 < len(pieces):
            s_next = score(idx + 1)
        top = jnp.max(s, axis=-1, keepdims=True)
        m_new = top if m is None else jnp.maximum(m, top)
        p = jnp.exp(s - m_new)
        psum = jnp.sum(p, axis=-1, keepdims=True)
        pv = dot(p.astype(BF16), v_refs[c][lo:lo + bk, :])
        if m is None:
            l, acc = psum, pv
        else:
            alpha = jnp.exp(m - m_new)
            l = l * alpha + psum
            acc = acc * alpha + pv
        m = m_new
    o_ref[...] = (acc / l).astype(BF16)
    lse_ref[...] = as_row(m + jnp.log(l))


def attention(q, ks, vs, joined, bq=512, bk=1024):
    s, hd = q.shape
    nc = len(ks)
    bq = min(bq, s)
    bk = min(bk, s)
    kv = [full((s, hd))] * (2 * nc)
    return call(
        functools.partial(attn_body, nc, bk),
        grid=(s // bq,),
        in_specs=[rows(bq, hd)] + kv + [pl.BlockSpec(memory_space=pl.ANY)],
        out_specs=[rows(bq, hd), pl.BlockSpec((8, bq), lambda i: (0, i))],
        out_shape=[jax.ShapeDtypeStruct(joined.shape, BF16), jax.ShapeDtypeStruct((8, s), F32)],
        input_output_aliases={1 + 2 * nc: 0},
        flops=4 * s * s * nc * hd,
        nbytes=2 * s * hd * (2 + 2 * nc),
        name="attn_fwd",
    )(q, *ks, *vs, joined)


def outproj_bwd_body(db_ref, w_ref, u_ref, o_ref, do_ref, delta_ref, dp_ref, gb_ref):
    hd = do_ref.shape[1]
    mlp = u_ref.shape[1]
    db = db_ref[...]
    do = dot(db, w_ref[:, :hd]).astype(BF16)
    do_ref[...] = do
    delta_ref[...] = as_row(jnp.sum(do.astype(F32) * o_ref[...].astype(F32), axis=-1, keepdims=True))

    @pl.when(pl.program_id(0) == 0)
    def _():
        gb_ref[...] = jnp.zeros_like(gb_ref)

    for lo in range(0, mlp, 256):
        dm = dot(db, w_ref[:, hd + lo:hd + lo + 256]).astype(BF16).astype(F32)
        u = u_ref[:, lo:lo + 256]
        u2 = u * u
        t = jnp.tanh(GELU_A * (u + GELU_B * (u2 * u)))
        grad = 0.5 * (1.0 + t) + 0.5 * u * (1.0 - t * t) * (GELU_A * (1.0 + 3.0 * GELU_B * u2))
        du = dm * grad
        gb_ref[:, lo:lo + 256] += jnp.sum(du, axis=0, keepdims=True)
        dp_ref[:, 3 * hd + lo:3 * hd + lo + 256] = du.astype(BF16)
    dp_ref[:, :3 * hd] = jnp.zeros((db.shape[0], 3 * hd), BF16)


def outproj_bwd(db, wt, u, joined):
    s, d = db.shape
    n = wt.shape[1]
    mlp = u.shape[1]
    hd = n - mlp
    tile = min(TILE, s)
    return call(
        outproj_bwd_body,
        grid=(s // tile,),
        in_specs=[rows(tile, d), full((d, n)), rows(tile, mlp), rows(tile, hd)],
        out_specs=[rows(tile, hd), pl.BlockSpec((8, tile), lambda i: (0, i)), rows(tile, 3 * hd + mlp), full((1, mlp))],
        out_shape=[jax.ShapeDtypeStruct((s, hd), BF16), jax.ShapeDtypeStruct((8, s), F32),
                   jax.ShapeDtypeStruct((s, 3 * hd + mlp), BF16), jax.ShapeDtypeStruct((1, mlp), F32)],
        flops=2 * s * d * n,
        nbytes=s * d * 2 + d * n * 2 + s * mlp * 4 + s * n * 3,
        name="outproj_bwd",
    )(db, wt, u, joined)


def attn_bwd_body(nc, bq, k_ref, v_ref, *refs):
    q_refs, do_refs, lse_refs, dl_refs = (refs[j * nc:(j + 1) * nc] for j in range(4))
    dq_refs, dk_ref, dv_ref = refs[4 * nc:5 * nc], refs[5 * nc], refs[5 * nc + 1]
    k = k_ref[...]
    v = v_ref[...]
    first = pl.program_id(0) == 0

    @pl.when(first)
    def _():
        for c in range(nc):
            dq_refs[c][...] = jnp.zeros_like(dq_refs[c])

    dk_ref[...] = jnp.zeros_like(dk_ref)
    dv_ref[...] = jnp.zeros_like(dv_ref)
    for c in range(nc):
        @pl.loop(0, q_refs[c].shape[0] // bq)
        def _(t, c=c):
            at = pl.ds(pl.multiple_of(t * bq, bq), bq)
            q = q_refs[c][at, :]
            do = do_refs[c][at, :]
            s = dot(k, q, ((1,), (1,)))
            dp = dot(v, do, ((1,), (1,)))
            p = jnp.exp(s - lse_refs[c][:1, at])
            dv_ref[...] += dot(p.astype(BF16), do)
            ds = (p * (dp - dl_refs[c][:1, at])).astype(BF16)
            dk_ref[...] += dot(ds, q)
            dq_refs[c][at, :] += dot(ds, k, ((0,), (0,)))


def attention_bwd(k, v, qs, dos, lses, deltas, bq=512, bk=512):
    s, hd = k.shape
    nc = len(qs)
    bq = min(bq, s)
    bk = min(bk, s)
    return call(
        functools.partial(attn_bwd_body, nc, bq),
        grid=(s // bk,),
        in_specs=[rows(bk, hd)] * 2 + [full((s, hd))] * (2 * nc) + [full((8, s))] * (2 * nc),
        out_specs=[full((s, hd))] * nc + [rows(bk, hd)] * 2,
        out_shape=[jax.ShapeDtypeStruct((s, hd), F32)] * (nc + 2),
        flops=10 * s * s * nc * hd,
        nbytes=2 * s * hd * (4 + 4 * nc),
        name="attn_bwd",
    )(k, v, *qs, *dos, *lses, *deltas)


def qk_bwd_body(nc, y_ref, cs_ref, qs_ref, ks_ref, *refs):
    dq_refs, dk_ref, dv_ref, _ = refs[:nc], refs[nc], refs[nc + 1], refs[nc + 2]
    dp_ref, gb_ref, gs_ref = refs[nc + 3:]
    hd = dk_ref.shape[1]
    half = hd // 2

    @pl.when(pl.program_id(0) == 0)
    def _():
        gb_ref[...] = jnp.zeros_like(gb_ref)
        gs_ref[...] = jnp.zeros_like(gs_ref)

    cos = cs_ref[:, :half]
    sin = cs_ref[:, half:]
    dq = dq_refs[0][...]
    for r in dq_refs[1:]:
        dq = dq + r[...]
    for part, (g, s_ref) in enumerate(((dq * hd ** -0.5, qs_ref), (dk_ref[...], ks_ref))):
        lo = part * hd
        y = y_ref[:, lo:lo + hd]
        inv = lax.rsqrt(jnp.mean(y * y, axis=-1, keepdims=True) + NORM_EPS)
        n = y * inv
        ga, gb = g[:, :half], g[:, half:]
        dt = jnp.concatenate([ga * cos + gb * sin, gb * cos - ga * sin], axis=1)
        gs_ref[:, lo:lo + hd] += jnp.sum(dt * n, axis=0, keepdims=True)
        dn = dt * s_ref[...]
        dy = inv * (dn - n * jnp.mean(dn * n, axis=-1, keepdims=True))
        gb_ref[:, lo:lo + hd] += jnp.sum(dy, axis=0, keepdims=True)
        dp_ref[:, lo:lo + hd] = dy.astype(BF16)
    dv = dv_ref[...]
    gb_ref[:, 2 * hd:] += jnp.sum(dv, axis=0, keepdims=True)
    dp_ref[:, 2 * hd:] = dv.astype(BF16)


def qk_bwd(yqk, cs, qs, ks, dqs, dk, dv, dproj):
    s, hd = dk.shape
    nc = len(dqs)
    tile = min(TILE, s)
    return call(
        functools.partial(qk_bwd_body, nc),
        grid=(s // tile,),
        in_specs=[rows(tile, 2 * hd), rows(tile, hd), full((1, hd)), full((1, hd))] + [rows(tile, hd)] * (nc + 2)
        + [pl.BlockSpec(memory_space=pl.ANY)],
        out_specs=[rows(tile, 3 * hd), full((1, 3 * hd)), full((1, 2 * hd))],
        out_shape=[jax.ShapeDtypeStruct(dproj.shape, BF16), jax.ShapeDtypeStruct((1, 3 * hd), F32), jax.ShapeDtypeStruct((1, 2 * hd), F32)],
        input_output_aliases={6 + nc: 0},
        flops=100 * s * hd,
        nbytes=s * hd * 4 * (6 + nc),
        name="qk_bwd",
    )(yqk, cs, qs, ks, *dqs, dk, dv, dproj)


def wgrad_body(nc, unsplit, *refs):
    a_refs, b_refs = refs[:nc], refs[nc:2 * nc]
    out_ref = refs[-1]
    acc = None
    for a, b in zip(a_refs, b_refs):
        part = dot(a[...], b[...], ((0,), (0,)))
        acc = part if acc is None else acc + part
    g = acc.astype(BF16)
    if unsplit:
        sel = refs[2 * nc][...]
        hd = sel.shape[0]
        for lo in (0, hd):
            out_ref[0, :, lo:lo + hd] = dot(g[:, lo:lo + hd], sel, ((1,), (1,))).astype(BF16)
        out_ref[0, :, 2 * hd:] = g[:, 2 * hd:]
    else:
        out_ref[0] = g


def wgrad(a_list, b_list, sel, block, num_blocks, prev, tile=256):
    nc = len(a_list)
    s, m = a_list[0].shape
    n = b_list[0].shape[1]
    args = list(a_list) + list(b_list)
    specs = [pl.BlockSpec((s, tile), lambda i: (0, i))] * nc
    specs += [pl.BlockSpec((s, n), lambda i: (0, 0), pipeline_mode=pl.Buffered(1))] * nc
    if sel is not None:
        args.append(sel)
        specs.append(full(sel.shape))
    alias = {}
    if prev is not None:
        alias = {len(args): 0}
        args.append(prev)
        specs.append(pl.BlockSpec(memory_space=pl.ANY))
    return call(
        functools.partial(wgrad_body, nc, sel is not None),
        grid=(m // tile,),
        in_specs=specs,
        out_specs=pl.BlockSpec((1, tile, n), lambda i: (block, i, 0)),
        out_shape=jax.ShapeDtypeStruct((num_blocks, m, n), BF16),
        input_output_aliases=alias,
        flops=2 * s * nc * m * n,
        nbytes=2 * (s * nc * (m + n) + m * n),
        name="wgrad_in" if sel is not None else "wgrad_out",
    )(*args)


def outer_body(col_ref, row_ref, *refs):
    refs[-1][0] = col_ref[...] * row_ref[...]


def outer(col, row, block, num_blocks, prev, tile=256):
    m, n = col.shape[0], row.shape[1]
    args = [col, row]
    specs = [rows(tile, 1), full((1, n))]
    alias = {}
    if prev is not None:
        alias = {2: 0}
        args.append(prev)
        specs.append(pl.BlockSpec(memory_space=pl.ANY))
    return call(
        outer_body,
        grid=(m // tile,),
        in_specs=specs,
        out_specs=pl.BlockSpec((1, tile, n), lambda i: (block, i, 0)),
        out_shape=jax.ShapeDtypeStruct((num_blocks, m, n), F32),
        input_output_aliases=alias,
        flops=50 * m * n,
        nbytes=4 * m * n,
        name="outer",
    )(*args)


def vec_sum_body(n, v_ref, o_ref, recv, send_sem, recv_sem):
    me = lax.axis_index("tp")
    barrier = pltpu.get_barrier_semaphore()
    for d in range(1, n):
        pl.semaphore_signal(barrier, inc=1, device_id={"tp": lax.rem(me + d, n)}, device_id_type=pl.DeviceIdType.MESH)
    pl.semaphore_wait(barrier, n - 1)
    sends = []
    for d in range(1, n):
        cp = pltpu.make_async_remote_copy(
            src_ref=v_ref, dst_ref=recv.at[me], send_sem=send_sem.at[d], recv_sem=recv_sem.at[me],
            device_id={"tp": lax.rem(me + d, n)}, device_id_type=pl.DeviceIdType.MESH)
        cp.start()
        sends.append(cp)
    recv[me] = v_ref[...]
    for d in range(1, n):
        src = lax.rem(me + d, n)
        pltpu.make_async_remote_copy(
            src_ref=v_ref, dst_ref=recv.at[src], send_sem=send_sem.at[d], recv_sem=recv_sem.at[src],
            device_id={"tp": src}, device_id_type=pl.DeviceIdType.MESH).wait_recv()
    total = recv[0]
    for d in range(1, n):
        total = total + recv[d]
    o_ref[...] = total
    for cp in sends:
        cp.wait_send()


def vec_sum(vec, n, cid):
    w = vec.shape[1]
    r = -(-w // LANES)
    r = -(-r // 8) * 8
    packed = jnp.pad(vec, ((0, 0), (0, r * LANES - w))).reshape(r, LANES)
    out = pl.pallas_call(
        functools.partial(vec_sum_body, n),
        in_specs=[pl.BlockSpec(memory_space=pltpu.VMEM)],
        out_specs=pl.BlockSpec(memory_space=pltpu.VMEM),
        out_shape=jax.ShapeDtypeStruct((r, LANES), F32),
        scratch_shapes=[pltpu.VMEM((n, r, LANES), F32), pltpu.SemaphoreType.DMA((n,)), pltpu.SemaphoreType.DMA((n,))],
        compiler_params=pltpu.CompilerParams(collective_id=cid, has_side_effects=True),
        cost_estimate=pl.CostEstimate(flops=10 ** 8, bytes_accessed=10 ** 6, transcendentals=0),
        name="vec_sum",
    )(packed)
    return out.reshape(1, r * LANES)[:, :w]


def layer_modulate(x_f32, mod_shift, mod_scale):
    row_mean = jnp.mean(x_f32, axis=-1, keepdims=True)
    centered = x_f32 - row_mean
    row_var = jnp.mean(centered * centered, axis=-1, keepdims=True)
    normed = centered * lax.rsqrt(row_var + NORM_EPS)
    return (normed * (1.0 + mod_scale) + mod_shift).astype(BF16)


def split_pairs(cols):
    src = lax.broadcasted_iota(jnp.int32, (cols, cols), 0)
    dst = lax.broadcasted_iota(jnp.int32, (cols, cols), 1)
    return (dst == src // 2 + (src % 2) * (cols // 2)).astype(BF16)


def unpair(vec):
    half = vec.shape[-1] // 2
    return jnp.stack([vec[..., :half], vec[..., half:]], axis=-1).reshape(vec.shape)


def pair(vec):
    return jnp.concatenate([vec[..., 0::2], vec[..., 1::2]], axis=-1)


def solution(mesh):
    act_spec = P("dp", "tp", None)
    in_specs = (act_spec, P("dp", None), P("tp", None), P("tp", None), P(None, None, None), P(None, None), P(None, None, "tp", None), P(None, "tp", None), P(None, None), P(None, None), P(None, "tp", None, None), P(None, None), act_spec)
    out_specs = (act_spec, act_spec, P("dp", None, None), P("dp", None), P("dp", None, "tp", None), P("dp", "tp", None), P("dp", None), P("dp", None), P("dp", "tp", None, None), P("dp", None))

    def device_fn(x_in, cond_vec, rope_cos, rope_sin, w_mod, b_mod, w_in, b_in, q_scale, k_scale, w_out, b_out, d_out):
        nb = w_in.shape[0]
        hd = q_scale.shape[1]
        nc = NUM_CHUNKS
        x_cur = x_in[0]
        ts, dim = x_cur.shape
        cw = ts // nc

        def gather(t):
            return [lax.all_gather(t[c * cw:(c + 1) * cw], "tp", axis=0, tiled=True) for c in range(nc)]

        def scatter(parts):
            return [lax.psum_scatter(p, "tp", scatter_dimension=0, tiled=True) for p in parts]

        silu_vec = jax.nn.silu(cond_vec.astype(F32)).astype(BF16)
        silu_col = silu_vec.astype(F32).reshape(-1, 1)
        n_tp = mesh.shape["tp"]
        sel = split_pairs(hd)
        cs_local = jnp.concatenate([rope_cos, rope_sin], axis=1).reshape(nc, cw, hd)
        cs = lax.all_gather(cs_local, "tp", axis=1, tiled=True)
        w_perm, b_perm, w_o, w_ot, qsc, ksc, mods = [], [], [], [], [], [], []

        def prepare(l, silu_vec, sel):
            mods.append(jnp.split(jnp.dot(silu_vec, w_mod[l], preferred_element_type=F32) + b_mod[l].astype(F32), 3, axis=-1))
            wl = w_in[l, :, 0, :]
            wq = jnp.dot(wl[:, :hd], sel, preferred_element_type=F32).astype(BF16)
            wk = jnp.dot(wl[:, hd:2 * hd], sel, preferred_element_type=F32).astype(BF16)
            w_perm.append(jnp.concatenate([wq, wk, wl[:, 2 * hd:]], axis=1))
            bl = b_in[l].astype(F32)
            b_perm.append(jnp.concatenate([pair(bl[:, :hd]), pair(bl[:, hd:2 * hd]), bl[:, 2 * hd:]], axis=1))
            w_o.append(w_out[l, 0])
            w_ot.append(w_out[l, 0].T)
            qsc.append(pair(q_scale[l:l + 1].astype(F32)))
            ksc.append(pair(k_scale[l:l + 1].astype(F32)))

        prepare(0, silu_vec, sel)
        saved = []
        for l in range(nb):
            shift, scale, gate = mods[l]
            x_f32 = x_cur.astype(F32)
            h = layer_modulate(x_f32, shift, scale)
            hf = gather(h)
            if l == nb - 1:
                gated_last = (d_out[0].astype(F32) * gate).astype(BF16)
                gated_last, hf[-1] = lax.optimization_barrier((gated_last, hf[-1]))
                db_last = gather(gated_last)
            proj = [inproj(hf[c], w_perm[l], b_perm[l], qsc[l], ksc[l], cs[c]) for c in range(nc)]
            if l + 1 < nb:
                prepare(l + 1, *lax.optimization_barrier((silu_vec, sel, proj[0][0]))[:2])
            qs, ks, vs, js, yqk, us = map(list, zip(*proj))
            lses, zs = [], []
            for c in range(nc):
                js[c], lse = attention(qs[c], ks, vs, js[c])
                lses.append(lse)
                zs.append(jnp.dot(js[c], w_o[l], preferred_element_type=F32).astype(BF16))
            if l == nb - 1:
                db_last[0], zs = lax.optimization_barrier((db_last[0], zs))
            mixed = jnp.concatenate(scatter(zs), axis=0)
            if l < nb - 1:
                branch = mixed.astype(F32) + b_out[l].astype(F32)
                x_cur = (x_f32 + gate * branch).astype(BF16)
            saved.append((x_f32, hf, qs, ks, vs, js, yqk, us, lses, mixed))

        grad_cur = d_out[0]
        grads = {}
        g_win = g_wout = g_wmod = None
        for l in reversed(range(nb)):
            x_f32, hf, qs, ks, vs, js, yqk, us, lses, mixed = saved[l]
            shift, scale, gate = mods[l]
            grad_f32 = grad_cur.astype(F32)
            gated = grad_f32 * gate
            d_bout = jnp.sum(gated, axis=0)
            db = db_last if l == nb - 1 else gather(gated.astype(BF16))
            if l < nb - 1:
                db[0], g_win, g_wout = lax.optimization_barrier((db[0], g_win, g_wout))
            back = [outproj_bwd(db[c], w_ot[l], us[c], js[c]) for c in range(nc)]
            dos, deltas, dprojs, gbu = map(list, zip(*back))
            dqs = [[] for _ in range(nc)]
            dks, dvs = [], []
            for c in range(nc):
                res = attention_bwd(ks[c], vs[c], qs, dos, lses, deltas)
                for e in range(nc):
                    dqs[e].append(res[e])
                dks.append(res[nc])
                dvs.append(res[nc + 1])
            gb3, gsc, dns = [], [], []
            for c in range(nc):
                dprojs[c], b3, s2 = qk_bwd(yqk[c], cs[c], qsc[l], ksc[l], dqs[c], dks[c], dvs[c], dprojs[c])
                gb3.append(b3)
                gsc.append(s2)
                dns.append(lax.dot_general(dprojs[c], w_perm[l], (((1,), (1,)), ((), ())), preferred_element_type=F32).astype(BF16))
            d_normed = scatter(dns)
            g_wout = wgrad(js, db, None, l, nb, g_wout)
            g_win = wgrad(hf, dprojs, sel, l, nb, g_win)
            d_normed, mixed, g_win = lax.optimization_barrier((d_normed, mixed, g_win))
            d_normed = jnp.concatenate(d_normed, axis=0)
            branch = mixed.astype(F32) + b_out[l].astype(F32)
            if l == nb - 1:
                x_out = (x_f32 + gate * branch).astype(BF16)
            gb3, gbu, gsc = sum(gb3), sum(gbu), sum(gsc)
            g_bin = jnp.concatenate([unpair(gb3[:, :hd]), unpair(gb3[:, hd:2 * hd]), gb3[:, 2 * hd:], gbu], axis=1)
            d_gate = jnp.sum(grad_f32 * branch, axis=0, keepdims=True)
            unused, norm_pull = jax.vjp(layer_modulate, x_f32, shift, scale)
            d_xnorm, d_shift, d_scale = norm_pull(d_normed)
            summed = vec_sum(jnp.concatenate([d_shift, d_scale, d_gate, d_bout[None], gsc], axis=1), n_tp, l)
            d_mod = summed[:, :3 * dim]
            g_wmod = outer(silu_col, d_mod, l, nb, g_wmod)
            d_qs = unpair(summed[0, 4 * dim:4 * dim + hd])
            d_ks = unpair(summed[0, 4 * dim + hd:])
            grads[l] = (d_mod[0], g_bin, d_qs, d_ks, summed[0, 3 * dim:4 * dim])
            grad_cur = (grad_f32 + d_xnorm).astype(BF16)
        g_bmod, g_bin, g_qs, g_ks, g_bout = (jnp.stack([grads[l][e] for l in range(nb)]) for e in range(5))
        return (x_out[None], grad_cur[None], g_wmod, g_bmod, g_win[:, :, None, :], g_bin, g_qs, g_ks, g_wout[:, None], g_bout)

    return jax.shard_map(device_fn, mesh=mesh, in_specs=in_specs, out_specs=out_specs, check_vma=False)
```

```python
import functools
import jax
import jax.numpy as jnp
from jax import lax
from jax.sharding import PartitionSpec as P
from jax.experimental import pallas as pl
from jax.experimental.pallas import tpu as pltpu

NORM_EPS = 1e-6
NUM_CHUNKS = 2
TILE = 512
F32 = jnp.float32
BF16 = jnp.bfloat16
LANES = 128
GELU_A = 0.7978845608028654
GELU_B = 0.044715


def call(body, **kw):
    flops = kw.pop("flops")
    nbytes = kw.pop("nbytes")
    kw["cost_estimate"] = pl.CostEstimate(flops=int(flops), bytes_accessed=int(nbytes), transcendentals=0)
    kw["compiler_params"] = pltpu.CompilerParams(dimension_semantics=("arbitrary",), vmem_limit_bytes=60 * 1024 * 1024)
    return pl.pallas_call(body, **kw)


def full(shape):
    return pl.BlockSpec(shape, lambda i: (0,) * len(shape))


def rows(tile, cols):
    return pl.BlockSpec((tile, cols), lambda i: (i, 0))


def dot(a, b, dims=((1,), (0,))):
    return lax.dot_general(a, b, (dims, ((), ())), preferred_element_type=F32)


def as_row(col):
    return jnp.broadcast_to(col, (col.shape[0], LANES)).T[:8]


def inproj_body(h_ref, w_ref, b_ref, qs_ref, ks_ref, cs_ref, q_ref, k_ref, v_ref, j_ref, yqk_ref, u_ref):
    hd = q_ref.shape[1]
    half = hd // 2
    h = h_ref[...]
    cos = cs_ref[:, :half]
    sin = cs_ref[:, half:]
    mlp = u_ref.shape[1]

    def proj(lo, width):
        return dot(h, w_ref[:, lo:lo + width]) + b_ref[:, lo:lo + width]

    def finish_qk(y, lo, s_ref, o_ref, post):
        yqk_ref[:, lo:lo + hd] = y
        inv = lax.rsqrt(jnp.mean(y * y, axis=-1, keepdims=True) + NORM_EPS)
        t = y * inv * s_ref[...]
        ta, tb = t[:, :half], t[:, half:]
        ra = (ta * cos - tb * sin).astype(BF16)
        rb = (ta * sin + tb * cos).astype(BF16)
        if post is not None:
            ra = ra * BF16(post)
            rb = rb * BF16(post)
        o_ref[:, :half] = ra
        o_ref[:, half:] = rb

    def finish_mlp(u, lo):
        u_ref[:, lo:lo + 256] = u
        g = 0.5 * u * (1.0 + jnp.tanh(GELU_A * (u + GELU_B * (u * u * u))))
        j_ref[:, hd + lo:hd + lo + 256] = g.astype(BF16)

    def finish_v(v):
        v_ref[...] = v.astype(BF16)
        j_ref[:, :hd] = jnp.zeros((h.shape[0], hd), BF16)

    steps = [(0, hd, lambda y: finish_qk(y, 0, qs_ref, q_ref, hd ** -0.5)),
             (hd, hd, lambda y: finish_qk(y, hd, ks_ref, k_ref, None))]
    steps += [(3 * hd + lo, 256, lambda u, lo=lo: finish_mlp(u, lo)) for lo in range(0, mlp, 256)]
    steps += [(2 * hd, hd, finish_v)]
    ahead = proj(*steps[0][:2])
    for idx, step in enumerate(steps):
        now = ahead
        if idx + 1 < len(steps):
            ahead = proj(*steps[idx + 1][:2])
        step[2](now)


def inproj(h, w, b, qs, ks, cs):
    s, d = h.shape
    n = w.shape[1]
    hd = qs.shape[1]
    mlp = n - 3 * hd
    tile = min(TILE, s)
    return call(
        inproj_body,
        grid=(s // tile,),
        in_specs=[rows(tile, d), full((d, n)), full((1, n)), full((1, hd)), full((1, hd)), rows(tile, hd)],
        out_specs=[rows(tile, hd)] * 3 + [rows(tile, hd + mlp), rows(tile, 2 * hd), rows(tile, mlp)],
        out_shape=[jax.ShapeDtypeStruct((s, hd), BF16)] * 3
        + [jax.ShapeDtypeStruct((s, hd + mlp), BF16), jax.ShapeDtypeStruct((s, 2 * hd), F32), jax.ShapeDtypeStruct((s, mlp), F32)],
        flops=2 * s * d * n,
        nbytes=s * d * 2 + d * n * 2 + s * n * 6,
        name="inproj",
    )(h, w, b, qs, ks, cs)


def attn_body(nc, bk, q_ref, *refs):
    k_refs, v_refs, _, o_ref, lse_ref = refs[:nc], refs[nc:2 * nc], refs[2 * nc], refs[2 * nc + 1], refs[2 * nc + 2]
    q = q_ref[...]
    pieces = [(c, lo) for c in range(nc) for lo in range(0, k_refs[0].shape[0], bk)]

    def score(idx):
        c, lo = pieces[idx]
        return dot(q, k_refs[c][lo:lo + bk, :], ((1,), (1,)))

    m = l = acc = None
    s_next = score(0)
    for idx, (c, lo) in enumerate(pieces):
        s = s_next
        if idx + 1 < len(pieces):
            s_next = score(idx + 1)
        top = jnp.max(s, axis=-1, keepdims=True)
        m_new = top if m is None else jnp.maximum(m, top)
        p = jnp.exp(s - m_new)
        psum = jnp.sum(p, axis=-1, keepdims=True)
        pv = dot(p.astype(BF16), v_refs[c][lo:lo + bk, :])
        if m is None:
            l, acc = psum, pv
        else:
            alpha = jnp.exp(m - m_new)
            l = l * alpha + psum
            acc = acc * alpha + pv
        m = m_new
    o_ref[...] = (acc / l).astype(BF16)
    lse_ref[...] = as_row(m + jnp.log(l))


def attention(q, ks, vs, joined, bq=512, bk=1024):
    s, hd = q.shape
    nc = len(ks)
    bq = min(bq, s)
    bk = min(bk, s)
    kv = [full((s, hd))] * (2 * nc)
    return call(
        functools.partial(attn_body, nc, bk),
        grid=(s // bq,),
        in_specs=[rows(bq, hd)] + kv + [pl.BlockSpec(memory_space=pl.ANY)],
        out_specs=[rows(bq, hd), pl.BlockSpec((8, bq), lambda i: (0, i))],
        out_shape=[jax.ShapeDtypeStruct(joined.shape, BF16), jax.ShapeDtypeStruct((8, s), F32)],
        input_output_aliases={1 + 2 * nc: 0},
        flops=4 * s * s * nc * hd,
        nbytes=2 * s * hd * (2 + 2 * nc),
        name="attn_fwd",
    )(q, *ks, *vs, joined)


def outproj_bwd_body(db_ref, w_ref, u_ref, o_ref, do_ref, delta_ref, dp_ref, gb_ref):
    hd = do_ref.shape[1]
    mlp = u_ref.shape[1]
    db = db_ref[...]

    @pl.when(pl.program_id(0) == 0)
    def _():
        gb_ref[...] = jnp.zeros_like(gb_ref)

    def part(lo):
        return dot(db, w_ref[:, hd + lo:hd + lo + 256])

    ahead = part(0)
    for lo in range(0, mlp, 256):
        dm = ahead.astype(BF16).astype(F32)
        ahead = part(lo + 256) if lo + 256 < mlp else dot(db, w_ref[:, :hd])
        u = u_ref[:, lo:lo + 256]
        u2 = u * u
        t = jnp.tanh(u * (GELU_A + (GELU_A * GELU_B) * u2))
        grad = 0.5 + 0.5 * t + (u * (1.0 - t * t)) * (0.5 * GELU_A + (1.5 * GELU_A * GELU_B) * u2)
        du = dm * grad
        gb_ref[:, lo:lo + 256] += jnp.sum(du, axis=0, keepdims=True)
        dp_ref[:, 3 * hd + lo:3 * hd + lo + 256] = du.astype(BF16)
    do = ahead.astype(BF16)
    do_ref[...] = do
    delta_ref[...] = as_row(jnp.sum(do.astype(F32) * o_ref[...].astype(F32), axis=-1, keepdims=True))


def outproj_bwd(db, wt, u, joined):
    s, d = db.shape
    n = wt.shape[1]
    mlp = u.shape[1]
    hd = n - mlp
    tile = min(TILE, s)
    return call(
        outproj_bwd_body,
        grid=(s // tile,),
        in_specs=[rows(tile, d), full((d, n)), rows(tile, mlp), rows(tile, hd)],
        out_specs=[rows(tile, hd), pl.BlockSpec((8, tile), lambda i: (0, i)), rows(tile, 3 * hd + mlp), full((1, mlp))],
        out_shape=[jax.ShapeDtypeStruct((s, hd), BF16), jax.ShapeDtypeStruct((8, s), F32),
                   jax.ShapeDtypeStruct((s, 3 * hd + mlp), BF16), jax.ShapeDtypeStruct((1, mlp), F32)],
        flops=2 * s * d * n,
        nbytes=s * d * 2 + d * n * 2 + s * mlp * 4 + s * n * 3,
        name="outproj_bwd",
    )(db, wt, u, joined)


def attn_bwd_body(nc, bq, k_ref, v_ref, *refs):
    q_refs, do_refs, lse_refs, dl_refs = (refs[j * nc:(j + 1) * nc] for j in range(4))
    dq_refs, dk_ref, dv_ref = refs[4 * nc:5 * nc], refs[5 * nc], refs[5 * nc + 1]
    k = k_ref[...]
    v = v_ref[...]
    first = pl.program_id(0) == 0

    @pl.when(first)
    def _():
        for c in range(nc):
            dq_refs[c][...] = jnp.zeros_like(dq_refs[c])

    pieces = [(c, t) for c in range(nc) for t in range(0, q_refs[0].shape[0], bq)]

    def start(idx):
        c, t = pieces[idx]
        q = q_refs[c][t:t + bq, :]
        do = do_refs[c][t:t + bq, :]
        return q, do, dot(k, q, ((1,), (1,))), dot(v, do, ((1,), (1,)))

    dk_sum = dv_sum = None
    ahead = start(0)
    for idx, (c, t) in enumerate(pieces):
        q, do, s, dp = ahead
        if idx + 1 < len(pieces):
            ahead = start(idx + 1)
        p = jnp.exp(s - lse_refs[c][:1, t:t + bq])
        ds = (p * (dp - dl_refs[c][:1, t:t + bq])).astype(BF16)
        dv_part = dot(p.astype(BF16), do)
        dk_part = dot(ds, q)
        dv_sum = dv_part if dv_sum is None else dv_sum + dv_part
        dk_sum = dk_part if dk_sum is None else dk_sum + dk_part
        dq_refs[c][t:t + bq, :] += dot(ds, k, ((0,), (0,)))
    dk_ref[...] = dk_sum
    dv_ref[...] = dv_sum


def attention_bwd(k, v, qs, dos, lses, deltas, bq=512, bk=512):
    s, hd = k.shape
    nc = len(qs)
    bq = min(bq, s)
    bk = min(bk, s)
    return call(
        functools.partial(attn_bwd_body, nc, bq),
        grid=(s // bk,),
        in_specs=[rows(bk, hd)] * 2 + [full((s, hd))] * (2 * nc) + [full((8, s))] * (2 * nc),
        out_specs=[full((s, hd))] * nc + [rows(bk, hd)] * 2,
        out_shape=[jax.ShapeDtypeStruct((s, hd), F32)] * (nc + 2),
        flops=10 * s * s * nc * hd,
        nbytes=2 * s * hd * (4 + 4 * nc),
        name="attn_bwd",
    )(k, v, *qs, *dos, *lses, *deltas)


def qk_bwd_body(nc, y_ref, cs_ref, qs_ref, ks_ref, *refs):
    dq_refs, dk_ref, dv_ref, _ = refs[:nc], refs[nc], refs[nc + 1], refs[nc + 2]
    dp_ref, gb_ref, gs_ref = refs[nc + 3:]
    hd = dk_ref.shape[1]
    half = hd // 2

    @pl.when(pl.program_id(0) == 0)
    def _():
        gb_ref[...] = jnp.zeros_like(gb_ref)
        gs_ref[...] = jnp.zeros_like(gs_ref)

    cos = cs_ref[:, :half]
    sin = cs_ref[:, half:]
    dq = dq_refs[0][...]
    for r in dq_refs[1:]:
        dq = dq + r[...]
    for part, (g, s_ref) in enumerate(((dq * hd ** -0.5, qs_ref), (dk_ref[...], ks_ref))):
        lo = part * hd
        y = y_ref[:, lo:lo + hd]
        inv = lax.rsqrt(jnp.mean(y * y, axis=-1, keepdims=True) + NORM_EPS)
        n = y * inv
        ga, gb = g[:, :half], g[:, half:]
        dt = jnp.concatenate([ga * cos + gb * sin, gb * cos - ga * sin], axis=1)
        gs_ref[:, lo:lo + hd] += jnp.sum(dt * n, axis=0, keepdims=True)
        dn = dt * s_ref[...]
        dy = inv * (dn - n * jnp.mean(dn * n, axis=-1, keepdims=True))
        gb_ref[:, lo:lo + hd] += jnp.sum(dy, axis=0, keepdims=True)
        dp_ref[:, lo:lo + hd] = dy.astype(BF16)
    dv = dv_ref[...]
    gb_ref[:, 2 * hd:] += jnp.sum(dv, axis=0, keepdims=True)
    dp_ref[:, 2 * hd:] = dv.astype(BF16)


def qk_bwd(yqk, cs, qs, ks, dqs, dk, dv, dproj):
    s, hd = dk.shape
    nc = len(dqs)
    tile = min(TILE, s)
    return call(
        functools.partial(qk_bwd_body, nc),
        grid=(s // tile,),
        in_specs=[rows(tile, 2 * hd), rows(tile, hd), full((1, hd)), full((1, hd))] + [rows(tile, hd)] * (nc + 2)
        + [pl.BlockSpec(memory_space=pl.ANY)],
        out_specs=[rows(tile, 3 * hd), full((1, 3 * hd)), full((1, 2 * hd))],
        out_shape=[jax.ShapeDtypeStruct(dproj.shape, BF16), jax.ShapeDtypeStruct((1, 3 * hd), F32), jax.ShapeDtypeStruct((1, 2 * hd), F32)],
        input_output_aliases={6 + nc: 0},
        flops=100 * s * hd,
        nbytes=s * hd * 4 * (6 + nc),
        name="qk_bwd",
    )(yqk, cs, qs, ks, *dqs, dk, dv, dproj)


def wgrad_body(nc, unsplit, *refs):
    a_refs, b_refs = refs[:nc], refs[nc:2 * nc]
    out_ref = refs[-1]
    acc = None
    for a, b in zip(a_refs, b_refs):
        part = dot(a[...], b[...], ((0,), (0,)))
        acc = part if acc is None else acc + part
    g = acc.astype(BF16)
    if unsplit:
        sel = refs[2 * nc][...]
        hd = sel.shape[0]
        for lo in (0, hd):
            out_ref[0, :, lo:lo + hd] = dot(g[:, lo:lo + hd], sel, ((1,), (1,))).astype(BF16)
        out_ref[0, :, 2 * hd:] = g[:, 2 * hd:]
    else:
        out_ref[0] = g


def wgrad(a_list, b_list, sel, block, num_blocks, prev, tile=256):
    nc = len(a_list)
    s, m = a_list[0].shape
    n = b_list[0].shape[1]
    args = list(a_list) + list(b_list)
    specs = [pl.BlockSpec((s, tile), lambda i: (0, i))] * nc
    specs += [pl.BlockSpec((s, n), lambda i: (0, 0), pipeline_mode=pl.Buffered(1))] * nc
    if sel is not None:
        args.append(sel)
        specs.append(full(sel.shape))
    alias = {}
    if prev is not None:
        alias = {len(args): 0}
        args.append(prev)
        specs.append(pl.BlockSpec(memory_space=pl.ANY))
    return call(
        functools.partial(wgrad_body, nc, sel is not None),
        grid=(m // tile,),
        in_specs=specs,
        out_specs=pl.BlockSpec((1, tile, n), lambda i: (block, i, 0)),
        out_shape=jax.ShapeDtypeStruct((num_blocks, m, n), BF16),
        input_output_aliases=alias,
        flops=2 * s * nc * m * n,
        nbytes=2 * (s * nc * (m + n) + m * n),
        name="wgrad_in" if sel is not None else "wgrad_out",
    )(*args)


def outer_body(col_ref, row_ref, *refs):
    refs[-1][0] = col_ref[...] * row_ref[...]


def outer(col, row, block, num_blocks, prev, tile=256):
    m, n = col.shape[0], row.shape[1]
    args = [col, row]
    specs = [rows(tile, 1), full((1, n))]
    alias = {}
    if prev is not None:
        alias = {2: 0}
        args.append(prev)
        specs.append(pl.BlockSpec(memory_space=pl.ANY))
    return call(
        outer_body,
        grid=(m // tile,),
        in_specs=specs,
        out_specs=pl.BlockSpec((1, tile, n), lambda i: (block, i, 0)),
        out_shape=jax.ShapeDtypeStruct((num_blocks, m, n), F32),
        input_output_aliases=alias,
        flops=50 * m * n,
        nbytes=4 * m * n,
        name="outer",
    )(*args)


def vec_sum_body(n, v_ref, o_ref, recv, send_sem, recv_sem):
    me = lax.axis_index("tp")
    barrier = pltpu.get_barrier_semaphore()
    for d in range(1, n):
        pl.semaphore_signal(barrier, inc=1, device_id={"tp": lax.rem(me + d, n)}, device_id_type=pl.DeviceIdType.MESH)
    pl.semaphore_wait(barrier, n - 1)
    sends = []
    for d in range(1, n):
        cp = pltpu.make_async_remote_copy(
            src_ref=v_ref, dst_ref=recv.at[me], send_sem=send_sem.at[d], recv_sem=recv_sem.at[me],
            device_id={"tp": lax.rem(me + d, n)}, device_id_type=pl.DeviceIdType.MESH)
        cp.start()
        sends.append(cp)
    recv[me] = v_ref[...]
    for d in range(1, n):
        src = lax.rem(me + d, n)
        pltpu.make_async_remote_copy(
            src_ref=v_ref, dst_ref=recv.at[src], send_sem=send_sem.at[d], recv_sem=recv_sem.at[src],
            device_id={"tp": src}, device_id_type=pl.DeviceIdType.MESH).wait_recv()
    total = recv[0]
    for d in range(1, n):
        total = total + recv[d]
    o_ref[...] = total
    for cp in sends:
        cp.wait_send()


def vec_sum(vec, n, cid):
    w = vec.shape[1]
    r = -(-w // LANES)
    r = -(-r // 8) * 8
    packed = jnp.pad(vec, ((0, 0), (0, r * LANES - w))).reshape(r, LANES)
    out = pl.pallas_call(
        functools.partial(vec_sum_body, n),
        in_specs=[pl.BlockSpec(memory_space=pltpu.VMEM)],
        out_specs=pl.BlockSpec(memory_space=pltpu.VMEM),
        out_shape=jax.ShapeDtypeStruct((r, LANES), F32),
        scratch_shapes=[pltpu.VMEM((n, r, LANES), F32), pltpu.SemaphoreType.DMA((n,)), pltpu.SemaphoreType.DMA((n,))],
        compiler_params=pltpu.CompilerParams(collective_id=cid, has_side_effects=True),
        cost_estimate=pl.CostEstimate(flops=10 ** 8, bytes_accessed=10 ** 6, transcendentals=0),
        name="vec_sum",
    )(packed)
    return out.reshape(1, r * LANES)[:, :w]


def layer_modulate(x_f32, mod_shift, mod_scale):
    row_mean = jnp.mean(x_f32, axis=-1, keepdims=True)
    centered = x_f32 - row_mean
    row_var = jnp.mean(centered * centered, axis=-1, keepdims=True)
    normed = centered * lax.rsqrt(row_var + NORM_EPS)
    return (normed * (1.0 + mod_scale) + mod_shift).astype(BF16)


def split_pairs(cols):
    src = lax.broadcasted_iota(jnp.int32, (cols, cols), 0)
    dst = lax.broadcasted_iota(jnp.int32, (cols, cols), 1)
    return (dst == src // 2 + (src % 2) * (cols // 2)).astype(BF16)


def unpair(vec):
    half = vec.shape[-1] // 2
    return jnp.stack([vec[..., :half], vec[..., half:]], axis=-1).reshape(vec.shape)


def pair(vec):
    return jnp.concatenate([vec[..., 0::2], vec[..., 1::2]], axis=-1)


def solution(mesh):
    act_spec = P("dp", "tp", None)
    in_specs = (act_spec, P("dp", None), P("tp", None), P("tp", None), P(None, None, None), P(None, None), P(None, None, "tp", None), P(None, "tp", None), P(None, None), P(None, None), P(None, "tp", None, None), P(None, None), act_spec)
    out_specs = (act_spec, act_spec, P("dp", None, None), P("dp", None), P("dp", None, "tp", None), P("dp", "tp", None), P("dp", None), P("dp", None), P("dp", "tp", None, None), P("dp", None))

    def device_fn(x_in, cond_vec, rope_cos, rope_sin, w_mod, b_mod, w_in, b_in, q_scale, k_scale, w_out, b_out, d_out):
        nb = w_in.shape[0]
        hd = q_scale.shape[1]
        nc = NUM_CHUNKS
        x_cur = x_in[0]
        ts, dim = x_cur.shape
        cw = ts // nc

        def gather(t):
            return [lax.all_gather(t[c * cw:(c + 1) * cw], "tp", axis=0, tiled=True) for c in range(nc)]

        def scatter(parts):
            return [lax.psum_scatter(p, "tp", scatter_dimension=0, tiled=True) for p in parts]

        silu_vec = jax.nn.silu(cond_vec.astype(F32)).astype(BF16)
        silu_col = silu_vec.astype(F32).reshape(-1, 1)
        n_tp = mesh.shape["tp"]
        sel = split_pairs(hd)
        cs_local = jnp.concatenate([rope_cos, rope_sin], axis=1).reshape(nc, cw, hd)
        cs = lax.all_gather(cs_local, "tp", axis=1, tiled=True)
        w_perm, b_perm, w_o, w_ot, qsc, ksc, mods = [], [], [], [], [], [], []

        def prepare(l, silu_vec, sel):
            mods.append(jnp.split(jnp.dot(silu_vec, w_mod[l], preferred_element_type=F32) + b_mod[l].astype(F32), 3, axis=-1))
            wl = w_in[l, :, 0, :]
            wq = jnp.dot(wl[:, :hd], sel, preferred_element_type=F32).astype(BF16)
            wk = jnp.dot(wl[:, hd:2 * hd], sel, preferred_element_type=F32).astype(BF16)
            w_perm.append(jnp.concatenate([wq, wk, wl[:, 2 * hd:]], axis=1))
            bl = b_in[l].astype(F32)
            b_perm.append(jnp.concatenate([pair(bl[:, :hd]), pair(bl[:, hd:2 * hd]), bl[:, 2 * hd:]], axis=1))
            w_o.append(w_out[l, 0])
            w_ot.append(w_out[l, 0].T)
            qsc.append(pair(q_scale[l:l + 1].astype(F32)))
            ksc.append(pair(k_scale[l:l + 1].astype(F32)))

        prepare(0, silu_vec, sel)
        saved = []
        for l in range(nb):
            shift, scale, gate = mods[l]
            x_f32 = x_cur.astype(F32)
            h = layer_modulate(x_f32, shift, scale)
            hf = gather(h)
            if l == nb - 1:
                gated_last = (d_out[0].astype(F32) * gate).astype(BF16)
                gated_last, hf[-1] = lax.optimization_barrier((gated_last, hf[-1]))
                db_last = gather(gated_last)
            proj = [inproj(hf[c], w_perm[l], b_perm[l], qsc[l], ksc[l], cs[c]) for c in range(nc)]
            if l + 1 < nb:
                prepare(l + 1, *lax.optimization_barrier((silu_vec, sel, proj[0][0]))[:2])
            qs, ks, vs, js, yqk, us = map(list, zip(*proj))
            lses, zs = [], []
            for c in range(nc):
                js[c], lse = attention(qs[c], ks, vs, js[c])
                lses.append(lse)
                zs.append(jnp.dot(js[c], w_o[l], preferred_element_type=F32).astype(BF16))
            if l == nb - 1:
                db_last[0], zs = lax.optimization_barrier((db_last[0], zs))
            mixed = scatter(zs)
            if l == 0 and nb > 1:
                prep = (w_perm[1], b_perm[1], mods[1], list(w_ot))
                mixed, (w_perm[1], b_perm[1], mods[1], w_ot[:]) = lax.optimization_barrier((mixed, prep))
            mixed = jnp.concatenate(mixed, axis=0)
            if l < nb - 1:
                branch = mixed.astype(F32) + b_out[l].astype(F32)
                x_cur = (x_f32 + gate * branch).astype(BF16)
            saved.append((x_f32, hf, qs, ks, vs, js, yqk, us, lses, mixed))

        grad_cur = d_out[0]
        grads = {}
        g_win = g_wout = g_wmod = None
        for l in reversed(range(nb)):
            x_f32, hf, qs, ks, vs, js, yqk, us, lses, mixed = saved[l]
            shift, scale, gate = mods[l]
            grad_f32 = grad_cur.astype(F32)
            gated = grad_f32 * gate
            d_bout = jnp.sum(gated, axis=0)
            db = db_last if l == nb - 1 else gather(gated.astype(BF16))
            if l < nb - 1:
                db[0], g_win, g_wout, g_wmod = lax.optimization_barrier((db[0], g_win, g_wout, g_wmod))
            back = [outproj_bwd(db[c], w_ot[l], us[c], js[c]) for c in range(nc)]
            dos, deltas, dprojs, gbu = map(list, zip(*back))
            dqs = [[] for _ in range(nc)]
            dks, dvs = [], []
            for c in range(nc):
                res = attention_bwd(ks[c], vs[c], qs, dos, lses, deltas)
                for e in range(nc):
                    dqs[e].append(res[e])
                dks.append(res[nc])
                dvs.append(res[nc + 1])
            gb3, gsc, dns = [], [], []
            for c in range(nc):
                dprojs[c], b3, s2 = qk_bwd(yqk[c], cs[c], qsc[l], ksc[l], dqs[c], dks[c], dvs[c], dprojs[c])
                gb3.append(b3)
                gsc.append(s2)
                dns.append(lax.dot_general(dprojs[c], w_perm[l], (((1,), (1,)), ((), ())), preferred_element_type=F32).astype(BF16))
            d_normed = scatter(dns)
            g_wout = wgrad(js, db, None, l, nb, g_wout)
            g_win = wgrad(hf, dprojs, sel, l, nb, g_win)
            d_normed, mixed, g_win = lax.optimization_barrier((d_normed, mixed, g_win))
            d_normed = jnp.concatenate(d_normed, axis=0)
            branch = mixed.astype(F32) + b_out[l].astype(F32)
            if l == nb - 1:
                x_out = (x_f32 + gate * branch).astype(BF16)
            gb3, gbu, gsc = sum(gb3), sum(gbu), sum(gsc)
            g_bin = jnp.concatenate([unpair(gb3[:, :hd]), unpair(gb3[:, hd:2 * hd]), gb3[:, 2 * hd:], gbu], axis=1)
            d_gate = jnp.sum(grad_f32 * branch, axis=0, keepdims=True)
            unused, norm_pull = jax.vjp(layer_modulate, x_f32, shift, scale)
            d_xnorm, d_shift, d_scale = norm_pull(d_normed)
            summed = vec_sum(jnp.concatenate([d_shift, d_scale, d_gate, d_bout[None], gsc], axis=1), n_tp, l)
            d_mod = summed[:, :3 * dim]
            g_wmod = outer(silu_col, d_mod, l, nb, g_wmod)
            d_qs = unpair(summed[0, 4 * dim:4 * dim + hd])
            d_ks = unpair(summed[0, 4 * dim + hd:])
            grads[l] = (d_mod[0], g_bin, d_qs, d_ks, summed[0, 3 * dim:4 * dim])
            grad_cur = (grad_f32 + d_xnorm).astype(BF16)
        g_bmod, g_bin, g_qs, g_ks, g_bout = (jnp.stack([grads[l][e] for l in range(nb)]) for e in range(5))
        return (x_out[None], grad_cur[None], g_wmod, g_bmod, g_win[:, :, None, :], g_bin, g_qs, g_ks, g_wout[:, None], g_bout)

    return jax.shard_map(device_fn, mesh=mesh, in_specs=in_specs, out_specs=out_specs, check_vma=False)
```
